32 devices in a mesh: dp: 16 (over z, y, x), expert: 2 (over core).
Axes of the slice: x: 2, y: 2, z: 4, core: 2. Of those that a mesh axis runs over, the one named last changes fastest.
Arguments:
- master: float32 [2, 7168, 2048], P('expert', 'dp'), may hold values from -6 to 6
- first_moment: float32 [2, 7168, 2048], P('expert', 'dp'), may hold values from -0.06 to 0.06
- second_moment: float32 [2, 7168, 2048], P('expert', 'dp'), may hold values from 1e-05 to 0.001
- rotation: int32 [4, 16, 1], replicated, may hold values from 0 to 15; in each aligned block of 16 rows (0 to 15, 16 to 31, ..., all dimensions but the last counted through in order) at most 3 rows name the same one
- assignment: int32 [64], replicated, may hold values from 0 to 63, each once
Outputs:
- saved_master: float32 [2, 64, 3, 1792, 128], P('expert', 'dp')
- saved_update: float32 [2, 64, 3, 1792, 128], P('expert', 'dp')
- checksums: float32 [2, 2, 64], replicated
The draws below stay inside these ranges and needn't reach their ends.
Inputs may be any that keep to these rules, and one draw needn't show every extreme that they name: rotation[r, j, 0] is the dp index that writes span j of round r; within one round no index is named more than 3 times, and in some round one index is named exactly 3 times. `assignment`: a permutation of the spans' checksum slots.
All inputs are finite; a program needn't handle non-finite values.
Results may differ from the reference program's by a relative error of at most 0.00002.
Values sent between devices are 32-bit elements; how exact they have to be, the bound alone decides.
No kernel may reach another device: no remote copies, remote signals or barrier semaphores. Data moves between devices by JAX's collectives and lax.ppermute only.
A program may use at most 128 MiB of HBM per device.

```python
import math
import jax
import jax.numpy as jnp
import numpy as np
from jax import lax

ROWS = 7168
COLS = 2048
LANE = 128
ROUNDS = 4
MOST = 3
STEP = 20
GROUPS = 2
SPANS = 64
N_DP = 16


def block_levels(stream_key, shape, pieces, smallest, top_value):
    gain, own = 1.0, jax.random.fold_in(stream_key, 6)
    for position, blocks in pieces:
        draws = jnp.exp(jax.random.uniform(jax.random.fold_in(own, position), (blocks,), jnp.float32, smallest / len(pieces), top_value / len(pieces)))
        gain = gain * jnp.repeat(draws, shape[position] // blocks).reshape([-1 if axis == position else 1 for axis in range(len(shape))])
    return gain


def shared_out(key, own, number, rows, count, top, bound, slope):
    ranking = jax.random.permutation(key, count)
    packed, usual = shares(count, rows * top, bound, slope, True), shares(count, rows * top, bound, slope, False)
    places = jnp.arange(count)

    def named(tallies, turn):
        used = int((tallies > 0).sum())
        fixed = max(1, used // 4)
        shifted = fixed + (places - fixed + turn * (used - fixed)) % max(1, count - fixed)
        return jnp.zeros((count,), jnp.int32).at[ranking[jnp.where(places < fixed, places, shifted)]].set(jnp.asarray(tallies, jnp.int32))

    tallies = jnp.where(number % 4 == 0, named(packed, number // 4), named(usual, number - number // 4 - 1))
    mixed = jax.random.permutation(jax.random.fold_in(own, 3), count)
    donor, sink = mixed[0:count // 2 * 2:2], mixed[1:count // 2 * 2:2]
    slack = jnp.minimum(tallies[donor] - 1, bound - tallies[sink]) // 2
    slack = jnp.where((donor == ranking[0]) | (sink == ranking[0]) | (tallies[sink] == 0), 0, jnp.maximum(slack, 0))
    shifted = jax.random.randint(jax.random.fold_in(own, 4), (count // 2,), 0, 1 << 20) % (slack + 1)
    tallies = tallies.at[donor].add(-shifted).at[sink].add(shifted)
    items = jnp.searchsorted(jnp.cumsum(tallies), jnp.arange(rows * top), side="right").astype(jnp.int32)
    listing = items.reshape(top, rows).T
    listing = listing[jax.random.permutation(jax.random.fold_in(own, 1), rows)]
    turn = jax.random.randint(jax.random.fold_in(own, 2), (rows, 1), 0, top)
    return jnp.take_along_axis(listing, (jnp.arange(top)[None, :] + turn) % top, axis=1)


def shares(amount, total, reach, slope, full):
    weights = [(1 << 20) // math.isqrt(standing ** slope) + 1 for standing in range(1, amount + 1)]
    largest = reach if full else min(reach, max(-(-total // amount), total * weights[0] // sum(weights)))
    least = 1 if total - largest >= amount - 1 else 0
    holding, rest = [largest] + [least] * (amount - 1), total - largest - least * (amount - 1)
    while rest > 0:
        movable = [i for i in range(1, amount) if holding[i] < largest] or [i for i in range(1, amount) if holding[i] < reach]
        whole, remaining = sum([weights[i] for i in movable]), rest
        for i in movable:
            extra = min(reach - holding[i], max(1, remaining * weights[i] // whole), rest)
            holding[i] = holding[i] + extra
            rest = rest - extra
    return np.array(holding)


def normal_values(rng, extent, deviation, reach, pieces=(), held_as=jnp.bfloat16):
    factor_of = block_levels(rng, extent, pieces, -0.22, 0.18) if pieces else 1.0
    drawn = jax.random.normal(rng, extent, jnp.float32) * deviation * factor_of
    return jnp.minimum(jnp.maximum(drawn, -reach), reach).astype(held_as)


def setup_inputs(seed: int = 0) -> dict:
    streams_of = jax.random.split(jax.random.key(seed), 6)
    master = normal_values(streams_of[0], (GROUPS, ROWS, COLS), 1.0, 6.0, ((0, 2), (1, 16)), jnp.float32)
    first_moment = normal_values(streams_of[1], (GROUPS, ROWS, COLS), 0.01, 0.06, ((0, 2), (1, 16)), jnp.float32)
    second_moment = jnp.clip(jnp.exp(math.log(0.001) - 4.6051703 * jax.random.uniform(streams_of[2], (GROUPS, ROWS, COLS), jnp.float32) ** block_levels(streams_of[2], (GROUPS, ROWS, COLS), ((0, 2), (1, 16)), -0.2, 0.2)), 9.999999747378752e-06, 0.001)
    rotation_keys = jax.random.split(jax.random.fold_in(streams_of[3], 1), ROUNDS * N_DP // N_DP)
    rotation_turns = jax.random.permutation(jax.random.fold_in(streams_of[3], 3), ROUNDS * N_DP // N_DP)
    rotation = jax.vmap(lambda own, number: shared_out(jax.random.fold_in(streams_of[3], 2), own, number, N_DP, N_DP, 1, MOST, 2))(rotation_keys, rotation_turns).reshape((ROUNDS, N_DP, 1))
    assignment = jax.random.permutation(streams_of[4], SPANS).astype(jnp.int32)
    return {"master": master, "first_moment": first_moment, "second_moment": second_moment, "rotation": rotation, "assignment": assignment}


BETA_ONE = 0.9
BETA_TWO = 0.95
EPSILON = 1e-08

def scaled_moment(first_part, second_part):
    corr_one = 1.0 - BETA_ONE ** STEP
    corr_two = 1.0 - BETA_TWO ** STEP
    return first_part / corr_one / (jnp.sqrt(second_part / corr_two) + EPSILON)

def slot_table(rotation, dp_count, most_slots):
    owners = rotation[:, :, 0]
    span_ids = jnp.arange(dp_count, dtype=jnp.int32)
    same_writer = owners[:, :, None] == owners[:, None, :]
    before = span_ids[None, :] < span_ids[:, None]
    slot_rank = lax.optimization_barrier(jnp.sum((same_writer & before[None]).astype(jnp.int32), axis=2))
    writers = jnp.arange(dp_count, dtype=jnp.int32)
    slot_ids = jnp.arange(most_slots, dtype=jnp.int32)
    matches = (owners[:, None, None, :] == writers[None, None, :, None]) & (slot_rank[:, None, None, :] == slot_ids[None, :, None, None])
    matches = matches.astype(jnp.int32)
    found_any = lax.optimization_barrier(jnp.sum(matches, axis=3))
    picked = lax.optimization_barrier(jnp.sum(matches * span_ids, axis=3))
    return (picked + (1 - found_any) * dp_count).astype(jnp.int32)

def position_weights(line_ids, per_row, lane_count):
    row_ids = line_ids // per_row
    col_ids = line_ids % per_row * lane_count
    lane_ids = jnp.arange(lane_count, dtype=jnp.int32)
    pattern = (row_ids[..., None] * 5 + (col_ids[..., None] + lane_ids) * 3) % 11
    return 1.0 + pattern.astype(jnp.float32) / 10.0

def reference(master, first_moment, second_moment, rotation, assignment):
    per_row = COLS // LANE
    lines_device = ROWS // N_DP * per_row
    piece_len = lines_device // (ROUNDS * N_DP)
    inv_count = 1.0 / math.sqrt(N_DP * piece_len * LANE)
    table = slot_table(rotation, N_DP, MOST)
    line_ids = jnp.arange(ROWS * per_row, dtype=jnp.int32).reshape(N_DP, ROUNDS, N_DP, piece_len)
    weights = position_weights(line_ids, per_row, LANE)
    round_ids = jnp.arange(ROUNDS, dtype=jnp.int32)[:, None, None]

    def arrange_field(field_in):
        line_view = field_in.reshape(N_DP, ROUNDS, N_DP, piece_len, LANE)
        totals = lax.optimization_barrier(jnp.sum(line_view * weights, axis=(0, 3, 4))) * inv_count
        reordered = jnp.transpose(line_view, (1, 2, 0, 3, 4))
        padded = jnp.concatenate([reordered, jnp.zeros((ROUNDS, 1, N_DP, piece_len, LANE), reordered.dtype)], axis=1)
        selected = padded[round_ids, table]
        saved_rows = jnp.transpose(selected, (2, 0, 1, 3, 4, 5)).reshape(N_DP * ROUNDS, MOST, N_DP * piece_len, LANE)
        return (saved_rows, totals.reshape(ROUNDS * N_DP))

    def one_group(fields):
        master_part, first_part, second_part = fields
        update = scaled_moment(first_part, second_part)
        saved_master, master_sums = arrange_field(master_part)
        saved_update, update_sums = arrange_field(update)
        return (saved_master, saved_update, jnp.stack([master_sums, update_sums]))
    saved_master, saved_update, group_sums = lax.map(one_group, (master, first_moment, second_moment))
    checksums = jnp.zeros_like(group_sums).at[:, :, assignment.astype(jnp.int32)].set(group_sums)
    return (saved_master, saved_update, checksums)
```

```python
import math

import jax
import jax.numpy as jnp
from jax import lax
from jax.experimental import pallas as pl
from jax.experimental.pallas import tpu as pltpu
from jax.sharding import PartitionSpec as P

LANE = 128
MOST = 3
STEP = 20
DIRECT = 6
SPARE = 8


BETA_ONE = 0.9
BETA_TWO = 0.95
EPSILON = 1e-08


def scaled_moment(first_part, second_part):
    corr_one = 1.0 - BETA_ONE**STEP
    corr_two = 1.0 - BETA_TWO**STEP
    return first_part / corr_one / (jnp.sqrt(second_part / corr_two) + EPSILON)


def position_weights(line_ids, per_row, lane_count):
    row_ids = line_ids // per_row
    col_ids = line_ids % per_row * lane_count
    lane_ids = jnp.arange(lane_count, dtype=jnp.int32)
    pattern = (row_ids[..., None] * 5 + (col_ids[..., None] + lane_ids) * 3) % 11
    return 1.0 + pattern.astype(jnp.float32) / 10.0


def span_plan(rotation, dp_count, direct, spare):
    owners = rotation.reshape(-1)
    span_total = owners.shape[0]
    ids = jnp.arange(span_total, dtype=jnp.int32)
    same = owners[:, None] == owners[None, :]
    before = ids[None, :] < ids[:, None]
    rank = jnp.sum((same & before).astype(jnp.int32), axis=1)
    in_round = ids[None, :] // dp_count == ids[:, None] // dp_count
    slot = jnp.sum((same & before & in_round).astype(jnp.int32), axis=1)
    late = rank >= direct
    late_rank = jnp.sum((late[None, :] & before).astype(jnp.int32), axis=1)
    late_total = jnp.sum(late.astype(jnp.int32))
    spare_ids = jnp.arange(spare, dtype=jnp.int32)
    late_spans = jnp.sum(
        jnp.where(late[None, :] & (late_rank[None, :] == spare_ids[:, None]), ids[None, :], 0), axis=1
    )
    return owners, rank, slot, late, late_rank, late_total, late_spans


def direct_table(owners, rank, dp_count, depth):
    ids = jnp.arange(owners.shape[0], dtype=jnp.int32)
    writers = jnp.arange(dp_count, dtype=jnp.int32)
    steps = jnp.arange(depth, dtype=jnp.int32)
    hit = (owners[None, None, :] == writers[:, None, None]) & (rank[None, None, :] == steps[None, :, None])
    return jnp.sum(jnp.where(hit, ids, 0), axis=2)


def placement(owners, rank, slot, late, late_rank, position, dp_count, round_count):
    ids = jnp.arange(owners.shape[0], dtype=jnp.int32)
    cells = jnp.arange(round_count * MOST, dtype=jnp.int32)
    hit = (
        (owners[None, :] == position)
        & (ids[None, :] // dp_count == cells[:, None] // MOST)
        & (slot[None, :] == cells[:, None] % MOST)
    )
    kind = jnp.sum(jnp.where(hit, 1 + late.astype(jnp.int32)[None, :], 0), axis=1)
    place = jnp.sum(jnp.where(hit & ~late[None, :], rank[None, :], 0), axis=1)
    late_place = jnp.sum(jnp.where(hit & late[None, :], late_rank[None, :], 0), axis=1)
    return kind, place, late_place


def assemble(kind, place, late_place, position, direct_buf, late_bufs):
    cell_count = kind.shape[0]
    dp_count, _, piece_len, lane_count = direct_buf.shape

    def kernel(kind_ref, place_ref, late_ref, pos_ref, direct_ref, *rest):
        late_refs, out_ref = rest[:-1], rest[-1]
        cell = pl.program_id(0)
        what = kind_ref[cell]

        @pl.when(what == 0)
        def _():
            out_ref[...] = jnp.zeros_like(out_ref)

        @pl.when(what == 1)
        def _():
            out_ref[0] = direct_ref[:, 0]

        @pl.when(what == 2)
        def _():
            for offset, late_ref_one in enumerate(late_refs):
                out_ref[0, pos_ref[0] ^ offset] = late_ref_one[0]

    in_specs = [
        pl.BlockSpec((dp_count, 1, piece_len, lane_count), lambda i, k, p, l, s: (0, p[i], 0, 0))
    ] + [
        pl.BlockSpec((1, piece_len, lane_count), lambda i, k, p, l, s: (l[i], 0, 0)) for _ in late_bufs
    ]
    return pl.pallas_call(
        kernel,
        out_shape=jax.ShapeDtypeStruct((cell_count, dp_count, piece_len, lane_count), direct_buf.dtype),
        grid_spec=pltpu.PrefetchScalarGridSpec(
            num_scalar_prefetch=4,
            grid=(cell_count,),
            in_specs=in_specs,
            out_specs=pl.BlockSpec(
                (1, dp_count, piece_len, lane_count), lambda i, k, p, l, s: (i, 0, 0, 0)
            ),
        ),
    )(kind, place, late_place, position.reshape(1), direct_buf, *late_bufs)


def swap(value, axis, size, bit):
    return lax.ppermute(value, axis, [(i, i ^ bit) for i in range(size)])


def hops(dp_count):
    order = sorted(range(1, dp_count), key=lambda d: bin(d).count("1"))
    return [d for d in order if d & 3 == 0], [d for d in order if d & 3]


def spread(got, offsets, dp_count):
    bits = dp_count.bit_length() - 1
    for offset in offsets:
        last = offset & -offset
        if bits >= 2 and offset & 3 == 3 and bin(offset >> 2).count("1") % 2:
            last = 2
        got[offset] = swap(got[offset ^ last], "dp", dp_count, last)
    return got


def shards(master, first_moment, second_moment, rotation, assignment):
    dp_count = lax.axis_size("dp")
    group_count = lax.axis_size("expert")
    position = lax.axis_index("dp")
    group_id = lax.axis_index("expert")
    round_count = rotation.shape[0]
    span_count = assignment.shape[0]
    rows_here = master.shape[1]
    lane_count = LANE
    per_row = master.shape[2] // lane_count
    lines_device = rows_here * per_row
    piece_len = lines_device // (round_count * dp_count)
    inv_count = 1.0 / math.sqrt(dp_count * piece_len * lane_count)
    most_total = round_count * MOST

    local_lines = position * lines_device + jnp.arange(lines_device, dtype=jnp.int32).reshape(
        span_count, piece_len
    )
    weights = position_weights(local_lines, per_row, lane_count)
    owners, rank, slot, late, late_rank, late_total, late_spans = span_plan(
        rotation, dp_count, DIRECT, SPARE
    )
    slot_ids = jnp.arange(span_count, dtype=jnp.int32)
    permuting = (assignment[:, None] == slot_ids[None, :]).astype(jnp.float32)
    in_slot = (jnp.arange(group_count, dtype=jnp.int32) == group_id).astype(jnp.float32)

    def terms(field_a, field_b):
        both = jnp.stack([jnp.sum(f * weights, axis=(1, 2)) * inv_count for f in (field_a, field_b)])
        placed = jnp.sum(both[:, :, None] * permuting[None], axis=1)
        return in_slot[:, None, None] * placed[None]

    def deliver(table, field_in, *after):
        if after:
            table = lax.optimization_barrier((table, *after))[0]
        send = field_in[table.reshape(-1)].reshape((dp_count, -1, piece_len, lane_count))
        return lax.all_to_all(send, "dp", split_axis=0, concat_axis=0, tiled=True)

    def lines(master_in, first_in, second_in):
        both = (master_in, scaled_moment(first_in, second_in))
        return tuple(f.reshape(span_count, piece_len, lane_count) for f in both)

    def quick(inputs):
        fields = lines(*inputs)
        table = direct_table(owners, rank, dp_count, DIRECT)
        cells = placement(owners, rank, slot, late, late_rank, position, dp_count, round_count)
        outer, inner = hops(dp_count)
        late_bufs = [spread({0: f[late_spans]}, outer, dp_count) for f in fields]
        far = [bufs[d] for bufs in late_bufs for d in outer]
        total = arrived = terms(*fields)
        bit = 1
        while bit < group_count:
            total = total + swap(total, "expert", group_count, bit)
            bit *= 2
        bit = 1
        while bit < dp_count:
            arrived = swap(total, "dp", dp_count, bit)
            total = total + arrived
            bit *= 2
        first_buf = deliver(table, fields[0], *far)
        spread(late_bufs[0], inner, dp_count)
        near = [late_bufs[0][d] for d in inner]
        second_buf = deliver(table, fields[1], arrived, *near)
        ordered = [late_bufs[0][d] for d in range(dp_count)]
        first_saved = assemble(*cells, position, first_buf, ordered)
        spread(late_bufs[1], inner[:-1], dp_count)
        parent = (inner[-1] ^ 1) if dp_count > 2 else 0
        held = inner[-1]
        source = late_bufs[1][parent]
        late_bufs[1][parent], first_saved = lax.optimization_barrier((source, first_saved))
        spread(late_bufs[1], [held], dp_count)
        ordered = [late_bufs[1][d] for d in range(dp_count)]
        saved = [first_saved, assemble(*cells, position, second_buf, ordered)]
        return saved[0], saved[1], total

    def padded(inputs):
        fields = lines(*inputs)
        table = direct_table(owners, rank, dp_count, most_total)
        never = jnp.zeros_like(late)
        cells = placement(owners, rank, slot, never, late_rank, position, dp_count, round_count)
        saved = [assemble(*cells, position, deliver(table, f), []) for f in fields]
        return saved[0], saved[1], lax.psum(terms(*fields), ("dp", "expert"))

    inputs = (master, first_moment, second_moment)
    if dp_count & (dp_count - 1) or group_count & (group_count - 1):
        saved_master, saved_update, checksums = padded(inputs)
    else:
        saved_master, saved_update, checksums = lax.cond(late_total <= SPARE, quick, padded, inputs)
    shape_out = (1, round_count, MOST, dp_count * piece_len, lane_count)
    return (saved_master.reshape(shape_out), saved_update.reshape(shape_out), checksums)


def solution(mesh):
    placed = (P("expert", "dp", None), P("expert", "dp", None), P("expert", "dp", None), P(), P())
    return jax.shard_map(
        shards,
        mesh=mesh,
        in_specs=placed,
        out_specs=(P("expert", "dp", None, None, None), P("expert", "dp", None, None, None), P()),
        check_vma=False,
    )
```
